32 devices in a mesh: tile: 8 (over z, y), mem: 4 (over x, core).
Axes of the slice: x: 2, y: 2, z: 4, core: 2. Of those that a mesh axis runs over, the one named last changes fastest.
Arguments:
- background: bfloat16 [112, 80, 512], P('tile', 'mem'), may hold values from -6 to 6
- obs_ens: bfloat16 [112, 80, 128], P('tile', 'mem'), may hold values from -6 to 6
- innovation: float32 [112, 128], P('tile'), may hold values from -6 to 6
- precision: float32 [112, 128], P('tile'), may hold values from 0.1 to 2
- loc_weight: float32 [112, 7], P('tile'), may hold values from 0.1 to 1
- old_split: int32 [9], replicated, may hold values from 0 to 64, as said below
- new_split: int32 [9], replicated, may hold values from 0 to 64, as said below
- obs_count: int32 [112], P('tile'), may hold values from 32 to 128
- halo_tiles: int32 [8, 12], replicated, may hold values from 0 to 63, as said below
- region_list: int32 [112, 7], P('tile'), may hold values from 0 to 25, as said below
Outputs:
- analysis: bfloat16 [112, 80, 512], P('tile', 'mem')
The draws below stay inside these ranges and needn't reach their ends.
Inputs may be any that keep to these rules, and one draw needn't show every extreme that they name: old_split[0] = 0 and old_split[8] = 64; each device holds between 2 and 14 old tiles, exactly 14 on some device. new_split[0] = 0 and new_split[8] = 64; each device holds between 6 and 10 new tiles; every new_split[d] differs from old_split[d] by at most 2, by exactly 2 for some d. `halo_tiles`: row d is 3 groups of 4 entries; a group holds distinct tiles in rising order that one device p other than d holds under new_split, with p within 3 of d, and the 3 devices of a row are distinct. `region_list`: for a slot of device d, an entry r < 14 names d's slot r, which is live; an entry r >= 14 names the tile halo_tiles[d, r - 14].
All inputs are finite; a program needn't handle non-finite values.
Results may differ from the reference program's by a relative error of at most 0.0057.
Values may be sent and summed in bfloat16 or wider, within the bound.
A program may use at most 64 MiB of HBM per device.

```python
import math
import jax
import jax.numpy as jnp
from jax import lax

MEMBERS = 80
STATE = 512
OBS_T = 128
TILE_MEAN = 8
CAP = 14
JITTER = 3
MOVE = 2
TILES = 64
SLOTS = 112
REACH = 3
HPEER = 3
HCAP = 4
HLIST = 12
NBR = 7
NS_ITERS = 6
N_TILE = 8


def split_pair(key):
    inner_key = jax.random.fold_in(key, 11)
    jitter_key, widest_key = jax.random.split(inner_key)
    boundary = jnp.arange(N_TILE + 1, dtype=jnp.int32)
    jitter = jax.random.randint(jitter_key, (N_TILE + 1,), -JITTER, JITTER + 1)
    widest = jax.random.randint(widest_key, (), 1, N_TILE - 1)
    jitter = jnp.where(boundary == widest, -JITTER, jitter)
    jitter = jnp.where(boundary == widest + 1, JITTER, jitter)
    jitter = jnp.where((boundary == 0) | (boundary == N_TILE), 0, jitter)
    old_bounds = boundary * TILE_MEAN + jitter
    moved_by = jnp.clip(jitter, -MOVE, MOVE)
    new_bounds = old_bounds - moved_by
    return (old_bounds.astype(jnp.int32), new_bounds.astype(jnp.int32))


def draw_old_split(key, part):
    return split_pair(key)[0]


def draw_new_split(key, part):
    return split_pair(key)[1]


def draw_halo_tiles(key, part):
    old_bounds, new_bounds = split_pair(key)
    inner_key = jax.random.fold_in(key, 23)
    peer_key, slot_key = jax.random.split(inner_key)
    offsets = jnp.concatenate([jnp.arange(-REACH, 0), jnp.arange(1, REACH + 1)]).astype(jnp.int32)
    device = jnp.arange(N_TILE, dtype=jnp.int32)
    target = device[:, None] + offsets[None, :]
    inside = (target >= 0) & (target < N_TILE)
    scores = jax.random.randint(peer_key, (N_TILE, 2 * REACH), 0, 1 << 20) * (2 * REACH) + jnp.arange(2 * REACH)[None, :]
    scores = jnp.where(inside, scores, (1 << 30) + jnp.arange(2 * REACH)[None, :])
    ranking = jnp.argsort(scores, axis=1, stable=True)[:, :HPEER]
    peer_ids = jnp.take_along_axis(target, ranking, axis=1)
    counts = new_bounds[1:] - new_bounds[:-1]
    peer_count = counts[peer_ids]
    slot_scores = jax.random.randint(slot_key, (N_TILE, HPEER, CAP), 0, 1 << 20) * CAP + jnp.arange(CAP)[None, None, :]
    slot_scores = jnp.where(jnp.arange(CAP)[None, None, :] < peer_count[:, :, None], slot_scores, (1 << 30) + jnp.arange(CAP)[None, None, :])
    chosen = jnp.sort(jnp.argsort(slot_scores, axis=2, stable=True)[:, :, :HCAP], axis=2)
    positions = new_bounds[peer_ids][:, :, None] + chosen
    return positions.reshape(N_TILE, HLIST).astype(jnp.int32)


def draw_region_list(key, part):
    old_bounds, new_bounds = split_pair(key)
    inner_key = jax.random.fold_in(key, 37)
    kind_key, own_key, far_key = jax.random.split(inner_key, 3)
    counts = new_bounds[1:] - new_bounds[:-1]
    count_per_slot = jnp.repeat(counts, CAP, total_repeat_length=N_TILE * CAP)
    own_pick = jax.random.randint(own_key, (N_TILE * CAP, NBR), 0, 1 << 20) % count_per_slot[:, None]
    far_pick = CAP + jax.random.randint(far_key, (N_TILE * CAP, NBR), 0, HLIST)
    choose_far = jax.random.randint(kind_key, (N_TILE * CAP, NBR), 0, 2)
    return jnp.where(choose_far == 1, far_pick, own_pick).astype(jnp.int32)


def place_ends(array, rng, low, high):
    longest = array.shape.index(max(array.shape))
    spots = []
    for shift in (0, 1):
        where = [jax.random.randint(jax.random.fold_in(rng, axis), (), 0, length) for axis, length in enumerate(array.shape)]
        where[longest] = (where[longest] + shift) % array.shape[longest]
        spots.append(tuple(where))
    return array.at[spots[0]].set(low).at[spots[1]].set(high)


def block_scale(rng, dims, pieces, least, high):
    loudness = 1.0
    for dim, parts in pieces:
        steps = jax.random.uniform(jax.random.fold_in(jax.random.fold_in(rng, 6), dim), (parts,), jnp.float32, least / len(pieces), high / len(pieces))
        loudness = loudness * jnp.repeat(jnp.exp(steps), dims[dim] // parts).reshape((-1,) + (1,) * (len(dims) - 1 - dim))
    return loudness


def noise(key, extent, scale, reach, cuts=(), held_as=jnp.bfloat16):
    level = block_scale(key, extent, cuts, -0.22, 0.18) if cuts else 1.0
    values = jax.random.normal(key, extent, jnp.float32) * scale * level
    return jnp.minimum(jnp.maximum(values, -reach), reach).astype(held_as)


def setup_inputs(seed: int = 0) -> dict:
    arg_keys = jax.random.split(jax.random.key(seed), 11)
    background = noise(arg_keys[0], (SLOTS, MEMBERS, STATE), 1.0, 6.0, ((0, 8), (1, 4)))
    obs_ens = noise(arg_keys[1], (SLOTS, MEMBERS, OBS_T), 1.0, 6.0, ((0, 8), (1, 4)))
    innovation = noise(arg_keys[2], (SLOTS, OBS_T), 1.0, 6.0, ((0, 8),), jnp.float32)
    precision = jnp.clip(jnp.exp(math.log(2.0) - 2.9957323 * jax.random.uniform(arg_keys[3], (SLOTS, OBS_T), jnp.float32) ** block_scale(arg_keys[3], (SLOTS, OBS_T), ((0, 8),), -0.2, 0.2)), 0.1, 2.0)
    loc_weight = jnp.clip(jnp.exp(math.log(1.0) - 2.3025851 * jax.random.uniform(arg_keys[4], (SLOTS, NBR), jnp.float32) ** block_scale(arg_keys[4], (SLOTS, NBR), ((0, 8),), -0.2, 0.2)), 0.1, 1.0)
    old_split = draw_old_split(jax.random.fold_in(arg_keys[10], 71), 0)
    new_split = draw_new_split(jax.random.fold_in(arg_keys[10], 71), 0)
    obs_count = place_ends(jax.random.randint(arg_keys[7], (SLOTS,), OBS_T // 4, OBS_T + 1), jax.random.fold_in(arg_keys[7], 1), OBS_T // 4, OBS_T).astype(jnp.int32)
    halo_tiles = draw_halo_tiles(jax.random.fold_in(arg_keys[10], 71), 0)
    region_list = draw_region_list(jax.random.fold_in(arg_keys[10], 71), 0)
    return dict(background=background, obs_ens=obs_ens, innovation=innovation, precision=precision, loc_weight=loc_weight, old_split=old_split, new_split=new_split, obs_count=obs_count, halo_tiles=halo_tiles, region_list=region_list)


inflation = 1.1
exact = lax.Precision.HIGHEST

def owner_of(split_points, position):
    bounds = split_points[1:]
    return lax.optimization_barrier(jnp.sum((bounds[None, :] <= position[:, None]).astype(jnp.int32), axis=1)).astype(jnp.int32)

def inverse_root(system, repeats):
    identity = jnp.eye(system.shape[-1], dtype=system.dtype)
    frobenius = jnp.sqrt(lax.optimization_barrier(jnp.sum(system * system, axis=(1, 2))))
    root_part = system / frobenius[:, None, None]
    inverse_part = jnp.broadcast_to(identity, system.shape)
    for repeat in range(repeats):
        middle = 0.5 * (3.0 * identity - jnp.einsum('pij,pjk->pik', inverse_part, root_part, precision=exact))
        root_part = jnp.einsum('pij,pjk->pik', root_part, middle, precision=exact)
        inverse_part = jnp.einsum('pij,pjk->pik', middle, inverse_part, precision=exact)
    return (inverse_part, frobenius)

def reference(background, obs_ens, innovation, precision, loc_weight, old_split, new_split, obs_count, halo_tiles, region_list):
    slot_all = jnp.arange(N_TILE * CAP, dtype=jnp.int32)
    device = (slot_all // CAP).astype(jnp.int32)
    within = (slot_all % CAP).astype(jnp.int32)
    tile_pos = new_split[device] + within
    live_slot = tile_pos < new_split[device + 1]
    safe_pos = jnp.minimum(tile_pos, TILES - 1).astype(jnp.int32)
    old_owner = owner_of(old_split, safe_pos)
    old_slot = (old_owner * CAP + safe_pos - old_split[old_owner]).astype(jnp.int32)
    live_obs = (jnp.arange(OBS_T, dtype=jnp.int32)[None, :] < obs_count[:, None]).astype(jnp.float32)
    root_weight = jnp.sqrt(precision * live_obs)
    scaled = (obs_ens.astype(jnp.float32) * root_weight[:, None, :]).astype(jnp.bfloat16)
    pulled = (root_weight * innovation).astype(jnp.bfloat16)
    flat_halo = halo_tiles.reshape(-1)
    halo_owner = owner_of(new_split, flat_halo)
    halo_slot = (halo_owner * CAP + flat_halo - new_split[halo_owner]).astype(jnp.int32).reshape(N_TILE, HLIST)
    own_slot = device[:, None] * CAP + region_list
    far_slot = halo_slot[device[:, None], jnp.clip(region_list - CAP, 0, HLIST - 1)]
    entry_slot = jnp.where(region_list < CAP, own_slot, far_slot).astype(jnp.int32)
    entry_slot = jnp.concatenate([slot_all[:, None], entry_slot], axis=1)
    entry_weight = jnp.concatenate([jnp.ones((N_TILE * CAP, 1), jnp.float32), loc_weight], axis=1)

    def one_device(device_index):
        slot_ids = (device_index * CAP + jnp.arange(CAP, dtype=jnp.int32)).astype(jnp.int32)
        region_rows = entry_slot[slot_ids]
        row_weights = entry_weight[slot_ids]
        region = scaled[region_rows].astype(jnp.float32)
        region_pulled = pulled[region_rows].astype(jnp.float32)
        products = jnp.einsum('pekn,pejn->pekj', region, region, precision=exact)
        gram_matrix = lax.optimization_barrier(jnp.sum(row_weights[:, :, None, None] * products, axis=1))
        pull_terms = jnp.einsum('pekn,pen->pek', region, region_pulled, precision=exact)
        pull_sum = lax.optimization_barrier(jnp.sum(row_weights[:, :, None] * pull_terms, axis=1))
        identity = jnp.eye(MEMBERS, dtype=jnp.float32)
        system = gram_matrix + (MEMBERS - 1) / inflation * identity
        inverse, frobenius = inverse_root(system, NS_ITERS)
        spread = (math.sqrt(MEMBERS - 1) / jnp.sqrt(frobenius))[:, None, None] * inverse
        half_way = jnp.einsum('pij,pj->pi', inverse, pull_sum, precision=exact)
        mean_weight = jnp.einsum('pij,pj->pi', inverse, half_way, precision=exact) / frobenius[:, None]
        transform = (spread + mean_weight[:, :, None]).astype(jnp.bfloat16).astype(jnp.float32)
        state_rows = background[old_slot[slot_ids]].astype(jnp.float32)
        mean_state = lax.optimization_barrier(jnp.sum(state_rows, axis=1)) / MEMBERS
        keep_share = 1.0 - lax.optimization_barrier(jnp.sum(transform, axis=1))
        analysis_rows = jnp.einsum('pij,pis->pjs', transform, state_rows, precision=exact) + keep_share[:, :, None] * mean_state[:, None, :]
        return jnp.where(live_slot[slot_ids][:, None, None], analysis_rows, 0.0).astype(jnp.bfloat16)
    result = lax.map(one_device, jnp.arange(N_TILE, dtype=jnp.int32))
    return result.reshape(N_TILE * CAP, MEMBERS, STATE)
```

```python
import functools
import math

import jax
import jax.numpy as jnp
from jax import lax
from jax.experimental import pallas as pl
from jax.experimental.pallas import tpu as pltpu
from jax.sharding import PartitionSpec as P

TILE_MEAN = 8
MOVE = 2
REACH = 3
HPEER = 3
HCAP = 4
NS_ITERS = 6
LIVE_MAX = TILE_MEAN + MOVE
INFLATION = 1.1
PAD = 32
MESH = pl.DeviceIdType.MESH
F32 = jnp.float32
BF16 = jnp.bfloat16
OFFSETS = tuple(range(-REACH, 0)) + tuple(range(1, REACH + 1))


def dot(a, b):
    return jnp.dot(a, b, preferred_element_type=F32)


def cut(a):
    high = a.astype(BF16)
    return high, (a - high.astype(F32)).astype(BF16)


def dot3(a, b):
    ah, al = a
    bh, bl = b
    return dot(ah, bh) + (dot(ah, bl) + dot(al, bh))


def kernel(
    devices,
    ranks,
    old_ref,
    new_ref,
    count_ref,
    halo_ref,
    region_ref,
    weight_ref,
    back_ref,
    obs_ref,
    innov_ref,
    prec_ref,
    out_ref,
    mine,
    table,
    stage,
    arrived,
    mig_out,
    mig_in,
    states,
    gram_s,
    y_s,
    z_s,
    t_out,
    t_in,
    halo_send,
    halo_recv,
    mig_send,
    mig_recv,
    own_send,
    own_recv,
    far_send,
    far_recv,
    state_send,
    state_recv,
    t_send,
    t_recv,
):
    capacity, members, width = back_ref.shape
    obs_slots = obs_ref.shape[2]
    ensemble = members * ranks
    full = PAD * ranks
    halo_count = HPEER * HCAP
    per_rank = -(-LIVE_MAX // ranks)
    me = lax.axis_index("tile")
    rank = lax.axis_index("mem")
    peers = [lax.rem(rank + j, ranks) for j in range(1, ranks)]

    barrier = pltpu.get_barrier_semaphore()
    for offset in OFFSETS:
        target = me + offset

        @pl.when((target >= 0) & (target < devices))
        def _():
            pl.semaphore_signal(barrier, inc=1, device_id=(target, rank), device_id_type=MESH)

    for peer in peers:
        pl.semaphore_signal(barrier, inc=1, device_id=(me, peer), device_id_type=MESH)

    old_start, old_end = old_ref[me], old_ref[me + 1]
    new_start, new_end = new_ref[me], new_ref[me + 1]
    row_id = lax.broadcasted_iota(jnp.int32, (PAD, obs_slots), 0)
    lane_id = lax.broadcasted_iota(jnp.int32, (1, obs_slots), 1)

    for s in range(LIVE_MAX):
        live = (lane_id < count_ref[s]).astype(F32)
        root = jnp.sqrt(prec_ref[s : s + 1, :] * live)
        pulled = root * innov_ref[s : s + 1, :]
        rows = obs_ref[s].astype(F32) * root
        fill = jnp.zeros((PAD - members, obs_slots), F32)
        block = jnp.concatenate([rows, fill], axis=0)
        block = jnp.where(row_id == members, pulled, block).astype(BF16)
        mine[s] = block
        table[s, rank] = block

    for k, offset in enumerate(OFFSETS):
        reader = jnp.clip(me + offset, 0, devices - 1)
        for c in range(HCAP):
            index = jnp.int32(0)
            for g in range(HPEER):
                first = halo_ref[reader, g * HCAP]
                here = (first >= new_start) & (first < new_end)
                index += jnp.where(here, halo_ref[reader, g * HCAP + c] - new_start, 0)
            index = jnp.clip(index, 0, LIVE_MAX - 1)
            stage[k, c] = mine[index]

    old_count = old_end - old_start
    for c in range(MOVE):
        mig_out[0, c] = back_ref[jnp.clip(c, 0, capacity - 1)]
        mig_out[1, c] = back_ref[jnp.clip(old_count - MOVE + c, 0, capacity - 1)]
    for s in range(LIVE_MAX):
        states[s, rank] = jnp.zeros((PAD, width), BF16)

    signals = ranks - 1
    for offset in OFFSETS:
        inside = (me + offset >= 0) & (me + offset < devices)
        signals += jnp.where(inside, 1, 0)
    pl.semaphore_wait(barrier, signals)

    def remote(src, dst, send, recv, target):
        return pltpu.make_async_remote_copy(
            src_ref=src,
            dst_ref=dst,
            send_sem=send,
            recv_sem=recv,
            device_id=target,
            device_id_type=MESH,
        )

    halo_copies = []
    for k, offset in enumerate(OFFSETS):
        target = me + offset
        back_slot = len(OFFSETS) - 1 - k
        copy = remote(
            stage.at[k], arrived.at[back_slot], halo_send.at[k], halo_recv.at[back_slot],
            (target, rank),
        )
        source = me + OFFSETS[back_slot]
        halo_copies.append(copy)

        @pl.when((target >= 0) & (target < devices))
        def _(copy=copy):
            copy.start()

    mig_copies = []
    for side, offset in ((0, -1), (1, 1)):
        target = me + offset
        copy = remote(
            mig_out.at[side], mig_in.at[1 - side], mig_send.at[side], mig_recv.at[1 - side],
            (target, rank),
        )
        mig_copies.append(copy)

        @pl.when((target >= 0) & (target < devices))
        def _(copy=copy):
            copy.start()

    own_rows = pl.ds(0, LIVE_MAX)
    far_rows = pl.ds(LIVE_MAX, halo_count)
    own_copies, far_copies, state_copies = [], [], []
    for j, peer in enumerate(peers):
        own = table.at[own_rows, rank]
        own_copies.append(remote(own, own, own_send.at[j], own_recv.at[j], (me, peer)))
        far = table.at[far_rows, rank]
        far_copies.append(remote(far, far, far_send.at[j], far_recv.at[j], (me, peer)))
        piece = states.at[:, rank]
        state_copies.append(remote(piece, piece, state_send.at[j], state_recv.at[j], (me, peer)))
    for copy in own_copies:
        copy.start()

    for k, offset in enumerate(OFFSETS):
        back_slot = len(OFFSETS) - 1 - k
        source = me + OFFSETS[back_slot]

        @pl.when((source >= 0) & (source < devices))
        def _(copy=halo_copies[k]):
            copy.wait_recv()

    for g in range(HPEER):
        first = halo_ref[me, g * HCAP]
        owner = jnp.int32(0)
        for k, offset in enumerate(OFFSETS):
            source = jnp.clip(me + offset, 0, devices - 1)
            held = (first >= new_ref[source]) & (first < new_ref[source + 1])
            inside = (me + offset >= 0) & (me + offset < devices)
            owner = jnp.where(held & inside, k, owner)
        for c in range(HCAP):
            table[LIVE_MAX + g * HCAP + c, rank] = arrived[owner, c]
    for copy in far_copies:
        copy.start()

    for side, offset in ((0, -1), (1, 1)):
        source = me - offset

        @pl.when((source >= 0) & (source < devices))
        def _(copy=mig_copies[side]):
            copy.wait_recv()

    for s in range(LIVE_MAX):
        position = new_start + s
        left = mig_in[0, jnp.clip(position - old_start + MOVE, 0, MOVE - 1)]
        own = back_ref[jnp.clip(position - old_start, 0, capacity - 1)]
        right = mig_in[1, jnp.clip(position - old_end, 0, MOVE - 1)]
        row = jnp.where(position < old_start, left, jnp.where(position < old_end, own, right))
        states[s, rank, :members] = row
    for copy in state_copies:
        copy.start()

    for copy in own_copies:
        copy.wait_recv()
    for copy in far_copies:
        copy.wait_recv()

    grid_row = lax.broadcasted_iota(jnp.int32, (full, full), 0)
    grid_col = lax.broadcasted_iota(jnp.int32, (full, full), 1)
    live_row = lax.rem(grid_row, PAD) < members
    live_col = lax.rem(grid_col, PAD) < members
    unit = (grid_row == grid_col).astype(F32)
    live_unit = jnp.where(live_row, unit, 0.0)
    line = lax.broadcasted_iota(jnp.int32, (1, full), 1)
    live_line = lax.rem(line, PAD) < members
    shift = (ensemble - 1) / INFLATION
    entries = region_ref.shape[1] + 1

    norms, pulls = [], []
    for b in range(per_rank):
        slot = jnp.minimum(rank + b * ranks, LIVE_MAX - 1)
        gram = jnp.zeros((full, full), F32)
        for e in range(entries):
            if e == 0:
                index = slot
            else:
                named = region_ref[slot, e - 1]
                index = jnp.where(named < capacity, named, named - capacity + LIVE_MAX)
            index = jnp.clip(index, 0, LIVE_MAX + halo_count - 1)
            block = table[index].reshape(full, obs_slots)
            product = lax.dot_general(
                block, block, (((1,), (1,)), ((), ())), preferred_element_type=F32
            )
            gram += product if e == 0 else weight_ref[slot, e - 1] * product
        pulls.append(jnp.where(live_line, gram[members : members + 1, :], 0.0))
        system = jnp.where(live_row & live_col, gram, 0.0) + shift * live_unit
        total = jnp.sum(jnp.sum(system * system, axis=1, keepdims=True), axis=0, keepdims=True)
        norm = jnp.sqrt(total)
        norms.append(norm)
        y = system / norm
        middle = 1.5 * unit - 0.5 * y
        y_s[b] = dot3(cut(y), cut(middle))
        z_s[b] = middle

    def step(_, carry):
        middles = []
        for b in range(per_rank):
            middles.append(cut(1.5 * unit - 0.5 * dot3(cut(z_s[b]), cut(y_s[b]))))
        for b in range(per_rank):
            y_s[b] = dot3(cut(y_s[b]), middles[b])
            z_s[b] = dot3(middles[b], cut(z_s[b]))
        return carry

    lax.fori_loop(0, NS_ITERS - 2, step, 0)
    for b in range(per_rank):
        z = cut(z_s[b])
        middle = cut(1.5 * unit - 0.5 * dot3(z, cut(y_s[b])))
        inverse = dot3(middle, z)
        parts = cut(inverse)
        pull = jnp.broadcast_to(pulls[b], (8, full))
        half = dot3(cut(pull), parts)
        shift_row = dot3(cut(half), parts)[:1] / norms[b]
        spread = math.sqrt(ensemble - 1) * lax.rsqrt(norms[b])
        transposed = spread * inverse + jnp.where(live_line, shift_row, 0.0)
        t_out[b] = transposed.astype(BF16).reshape(ranks, PAD, full)

    t_copies = []
    for j, peer in enumerate(peers):
        copy = remote(
            t_out.at[:, peer], t_in.at[rank], t_send.at[j], t_recv.at[j], (me, peer)
        )
        t_copies.append(copy)
        copy.start()
    t_in[rank] = t_out[:, rank]

    for copy in state_copies:
        copy.wait_recv()
    for copy in t_copies:
        copy.wait_recv()

    piece_row = lax.broadcasted_iota(jnp.int32, (PAD, full), 0)
    for s in range(LIVE_MAX):
        weights = t_in[s % ranks, s // ranks]
        weights = jnp.where(piece_row == members, jnp.ones_like(weights), weights)
        keep = 1.0 - jnp.sum(weights.astype(F32), axis=1, keepdims=True)
        blended = dot(weights, states[s].reshape(full, width))
        mean = blended[members : members + 1, :] / ensemble
        value = (blended + keep * mean)[:members]
        is_live = new_start + s < new_end
        out_ref[s] = jnp.where(is_live, value, 0.0).astype(BF16)
    for s in range(LIVE_MAX, capacity):
        out_ref[s] = jnp.zeros((members, width), BF16)

    for k, offset in enumerate(OFFSETS):
        target = me + offset

        @pl.when((target >= 0) & (target < devices))
        def _(copy=halo_copies[k]):
            copy.wait_send()

    for side, offset in ((0, -1), (1, 1)):
        target = me + offset

        @pl.when((target >= 0) & (target < devices))
        def _(copy=mig_copies[side]):
            copy.wait_send()

    for copy in own_copies + far_copies + state_copies + t_copies:
        copy.wait_send()


def shards(devices, ranks, background, obs_ens, innovation, precision, loc_weight, old_split,
           new_split, obs_count, halo_tiles, region_list):
    capacity, members, width = background.shape
    obs_slots = obs_ens.shape[2]
    full = PAD * ranks
    halo_count = HPEER * HCAP
    per_rank = -(-LIVE_MAX // ranks)
    smem = pl.BlockSpec(memory_space=pltpu.SMEM)
    vmem = pl.BlockSpec(memory_space=pltpu.VMEM)
    count = len(OFFSETS)
    dma = pltpu.SemaphoreType.DMA
    return pl.pallas_call(
        functools.partial(kernel, devices, ranks),
        out_shape=jax.ShapeDtypeStruct((capacity, members, width), BF16),
        in_specs=[smem] * 6 + [vmem] * 4,
        out_specs=vmem,
        scratch_shapes=[
            pltpu.VMEM((LIVE_MAX, PAD, obs_slots), BF16),
            pltpu.VMEM((LIVE_MAX + halo_count, ranks, PAD, obs_slots), BF16),
            pltpu.VMEM((count, HCAP, PAD, obs_slots), BF16),
            pltpu.VMEM((count, HCAP, PAD, obs_slots), BF16),
            pltpu.VMEM((2, MOVE, members, width), BF16),
            pltpu.VMEM((2, MOVE, members, width), BF16),
            pltpu.VMEM((LIVE_MAX, ranks, PAD, width), BF16),
            pltpu.VMEM((per_rank, full, full), F32),
            pltpu.VMEM((per_rank, full, full), F32),
            pltpu.VMEM((per_rank, full, full), F32),
            pltpu.VMEM((per_rank, ranks, PAD, full), BF16),
            pltpu.VMEM((ranks, per_rank, PAD, full), BF16),
            dma((count,)),
            dma((count,)),
            dma((2,)),
            dma((2,)),
            dma((ranks - 1,)),
            dma((ranks - 1,)),
            dma((ranks - 1,)),
            dma((ranks - 1,)),
            dma((ranks - 1,)),
            dma((ranks - 1,)),
            dma((ranks - 1,)),
            dma((ranks - 1,)),
        ],
        compiler_params=pltpu.CompilerParams(collective_id=0, has_side_effects=True),
        cost_estimate=pl.CostEstimate(flops=10**8, bytes_accessed=10**7, transcendentals=0),
    )(old_split, new_split, obs_count, halo_tiles, region_list, loc_weight, background, obs_ens,
      innovation, precision)


def solution(mesh):
    in_specs = (
        P("tile", "mem", None),
        P("tile", "mem", None),
        P("tile", None),
        P("tile", None),
        P("tile", None),
        P(),
        P(),
        P("tile"),
        P(),
        P("tile", None),
    )
    out_specs = P("tile", "mem", None)
    body = functools.partial(shards, mesh.shape["tile"], mesh.shape["mem"])
    return jax.shard_map(body, mesh=mesh, in_specs=in_specs, out_specs=out_specs, check_vma=False)
```

```python
import functools
import math

import jax
import jax.numpy as jnp
from jax import lax
from jax.experimental import pallas as pl
from jax.experimental.pallas import tpu as pltpu
from jax.sharding import PartitionSpec as P

TILE_MEAN = 8
MOVE = 2
REACH = 3
HPEER = 3
HCAP = 4
NS_ITERS = 6
LIVE_MAX = TILE_MEAN + MOVE
INFLATION = 1.1
PAD = 24
MESH = pl.DeviceIdType.MESH
F32 = jnp.float32
BF16 = jnp.bfloat16
OFFSETS = tuple(range(-REACH, 0)) + tuple(range(1, REACH + 1))


def dot(a, b):
    return jnp.dot(a, b, preferred_element_type=F32)


def cut(a):
    high = a.astype(BF16)
    return high, (a - high.astype(F32)).astype(BF16)


def dot3(a, b):
    ah, al = a
    bh, bl = b
    return dot(ah, bh) + (dot(ah, bl) + dot(al, bh))


def kernel(
    devices,
    ranks,
    old_ref,
    new_ref,
    count_ref,
    halo_ref,
    region_ref,
    weight_ref,
    back_ref,
    obs_ref,
    innov_ref,
    prec_ref,
    out_ref,
    mine,
    back_t,
    table,
    stage,
    arrived,
    mig_out,
    mig_in,
    states,
    gram_s,
    y_s,
    z_s,
    t_out,
    t_in,
    halo_send,
    halo_recv,
    mig_send,
    mig_recv,
    own_send,
    own_recv,
    far_send,
    far_recv,
    state_send,
    state_recv,
    t_send,
    t_recv,
):
    members, capacity, width = back_ref.shape
    obs_slots = obs_ref.shape[2]
    ensemble = members * ranks
    full = PAD * ranks
    halo_count = HPEER * HCAP
    per_rank = -(-LIVE_MAX // ranks)
    me = lax.axis_index("tile")
    rank = lax.axis_index("mem")
    peers = [lax.rem(rank + j, ranks) for j in range(1, ranks)]

    barrier = pltpu.get_barrier_semaphore()
    for offset in OFFSETS:
        target = me + offset

        @pl.when((target >= 0) & (target < devices))
        def _():
            pl.semaphore_signal(barrier, inc=1, device_id=(target, rank), device_id_type=MESH)

    for peer in peers:
        pl.semaphore_signal(barrier, inc=1, device_id=(me, peer), device_id_type=MESH)

    old_start, old_end = old_ref[me], old_ref[me + 1]
    new_start, new_end = new_ref[me], new_ref[me + 1]
    row_id = lax.broadcasted_iota(jnp.int32, (PAD, obs_slots), 0)
    lane_id = lax.broadcasted_iota(jnp.int32, (1, obs_slots), 1)

    obs_all = obs_ref[...].astype(F32)
    for s in range(LIVE_MAX):
        live = (lane_id < count_ref[s]).astype(F32)
        root = jnp.sqrt(prec_ref[s : s + 1, :] * live)
        pulled = root * innov_ref[s : s + 1, :]
        rows = obs_all[:, s, :] * root
        fill = jnp.zeros((PAD - members, obs_slots), F32)
        block = jnp.concatenate([rows, fill], axis=0)
        block = jnp.where(row_id == members, pulled, block).astype(BF16)
        mine[s] = block
        table[s, rank] = block

    for k, offset in enumerate(OFFSETS):
        reader = jnp.clip(me + offset, 0, devices - 1)
        for c in range(HCAP):
            index = jnp.int32(0)
            for g in range(HPEER):
                first = halo_ref[reader, g * HCAP]
                here = (first >= new_start) & (first < new_end)
                index += jnp.where(here, halo_ref[reader, g * HCAP + c] - new_start, 0)
            index = jnp.clip(index, 0, LIVE_MAX - 1)
            stage[k, c] = mine[index]

    for s in range(LIVE_MAX):
        states[s, rank] = jnp.zeros((PAD, width), BF16)

    signals = ranks - 1
    for offset in OFFSETS:
        inside = (me + offset >= 0) & (me + offset < devices)
        signals += jnp.where(inside, 1, 0)
    pl.semaphore_wait(barrier, signals)

    def remote(src, dst, send, recv, target):
        return pltpu.make_async_remote_copy(
            src_ref=src,
            dst_ref=dst,
            send_sem=send,
            recv_sem=recv,
            device_id=target,
            device_id_type=MESH,
        )

    halo_copies = []
    for k, offset in enumerate(OFFSETS):
        target = me + offset
        back_slot = len(OFFSETS) - 1 - k
        copy = remote(
            stage.at[k], arrived.at[back_slot], halo_send.at[k], halo_recv.at[back_slot],
            (target, rank),
        )
        source = me + OFFSETS[back_slot]
        halo_copies.append(copy)

        @pl.when((target >= 0) & (target < devices))
        def _(copy=copy):
            copy.start()

    own_rows = pl.ds(0, LIVE_MAX)
    far_rows = pl.ds(LIVE_MAX, halo_count)
    pair = rank + 1 - 2 * lax.rem(rank, 2)
    half_ranks = ranks // 2

    def gather(piece, send, recv):
        here = piece(rank)
        direct = [remote(here, here, send.at[0], recv.at[0], (me, pair))]
        passed = []
        for j in range(1, half_ranks):
            ahead = lax.rem(rank + 2 * j, ranks)
            behind = piece(lax.rem(rank + ranks - 2 * j, ranks))
            direct.append(remote(here, here, send.at[j], recv.at[j], (me, ahead)))
            k = half_ranks + j - 1
            passed.append(remote(behind, behind, send.at[k], recv.at[k], (me, pair)))
        return direct, passed

    def start(copies):
        for copy in copies:
            copy.start()

    def arrive(copies):
        for copy in copies:
            copy.wait_recv()

    own_copies, own_passed = gather(lambda r: table.at[own_rows, r], own_send, own_recv)
    far_copies, far_passed = gather(lambda r: table.at[far_rows, r], far_send, far_recv)
    state_copies, state_passed = gather(lambda r: states.at[:, r], state_send, state_recv)
    start(own_copies[::-1])

    back_all = back_ref[...].astype(F32)
    for s in range(capacity):
        back_t[s] = back_all[:, s, :].astype(BF16)
    old_count = old_end - old_start
    for c in range(MOVE):
        mig_out[0, c] = back_t[jnp.clip(c, 0, capacity - 1)]
        mig_out[1, c] = back_t[jnp.clip(old_count - MOVE + c, 0, capacity - 1)]
    mig_copies = []
    for side, offset in ((0, -1), (1, 1)):
        target = me + offset
        copy = remote(
            mig_out.at[side], mig_in.at[1 - side], mig_send.at[side], mig_recv.at[1 - side],
            (target, rank),
        )
        mig_copies.append(copy)

        @pl.when((target >= 0) & (target < devices))
        def _(copy=copy):
            copy.start()

    for k, offset in enumerate(OFFSETS):
        back_slot = len(OFFSETS) - 1 - k
        source = me + OFFSETS[back_slot]

        @pl.when((source >= 0) & (source < devices))
        def _(copy=halo_copies[k]):
            copy.wait_recv()

    for g in range(HPEER):
        first = halo_ref[me, g * HCAP]
        owner = jnp.int32(0)
        for k, offset in enumerate(OFFSETS):
            source = jnp.clip(me + offset, 0, devices - 1)
            held = (first >= new_ref[source]) & (first < new_ref[source + 1])
            inside = (me + offset >= 0) & (me + offset < devices)
            owner = jnp.where(held & inside, k, owner)
        for c in range(HCAP):
            table[LIVE_MAX + g * HCAP + c, rank] = arrived[owner, c]
    start(far_copies[::-1])

    for side, offset in ((0, -1), (1, 1)):
        source = me - offset

        @pl.when((source >= 0) & (source < devices))
        def _(copy=mig_copies[side]):
            copy.wait_recv()

    for s in range(LIVE_MAX):
        position = new_start + s
        left = mig_in[0, jnp.clip(position - old_start + MOVE, 0, MOVE - 1)]
        own = back_t[jnp.clip(position - old_start, 0, capacity - 1)]
        right = mig_in[1, jnp.clip(position - old_end, 0, MOVE - 1)]
        row = jnp.where(position < old_start, left, jnp.where(position < old_end, own, right))
        states[s, rank, :members] = row
    start(state_copies[::-1])

    arrive(own_copies[1:])
    start(own_passed)
    arrive(far_copies[1:])
    start(far_passed)
    arrive(own_copies[:1] + own_passed + far_copies[:1] + far_passed)

    grid_row = lax.broadcasted_iota(jnp.int32, (full, full), 0)
    grid_col = lax.broadcasted_iota(jnp.int32, (full, full), 1)
    live_row = lax.rem(grid_row, PAD) < members
    live_col = lax.rem(grid_col, PAD) < members
    unit = (grid_row == grid_col).astype(F32)
    live_unit = jnp.where(live_row, unit, 0.0)
    line = lax.broadcasted_iota(jnp.int32, (1, full), 1)
    live_line = lax.rem(line, PAD) < members
    shift = (ensemble - 1) / INFLATION
    entries = region_ref.shape[0] + 1

    norms, pulls = [], []
    for b in range(per_rank):
        slot = jnp.minimum(rank + b * ranks, LIVE_MAX - 1)
        gram = jnp.zeros((full, full), F32)
        for e in range(entries):
            if e == 0:
                index = slot
            else:
                named = region_ref[e - 1, slot]
                index = jnp.where(named < capacity, named, named - capacity + LIVE_MAX)
            index = jnp.clip(index, 0, LIVE_MAX + halo_count - 1)
            block = table[index].reshape(full, obs_slots)
            product = lax.dot_general(
                block, block, (((1,), (1,)), ((), ())), preferred_element_type=F32
            )
            gram += product if e == 0 else weight_ref[e - 1, slot] * product
        pulls.append(jnp.where(live_line, gram[members : members + 1, :], 0.0))
        system = jnp.where(live_row & live_col, gram, 0.0) + shift * live_unit
        total = jnp.sum(jnp.sum(system * system, axis=1, keepdims=True), axis=0, keepdims=True)
        norm = jnp.sqrt(total)
        norms.append(norm)
        y = system / norm
        middle = 1.5 * unit - 0.5 * y
        y_s[b] = dot3(cut(y), cut(middle))
        z_s[b] = middle

    def step(_, carry):
        middles = []
        for b in range(per_rank):
            middles.append(cut(1.5 * unit - 0.5 * dot3(cut(z_s[b]), cut(y_s[b]))))
        for b in range(per_rank):
            y_s[b] = dot3(cut(y_s[b]), middles[b])
            z_s[b] = dot3(middles[b], cut(z_s[b]))
        return carry

    lax.fori_loop(0, NS_ITERS - 2, step, 0)
    for b in range(per_rank):
        z = cut(z_s[b])
        middle = cut(1.5 * unit - 0.5 * dot3(z, cut(y_s[b])))
        inverse = dot3(middle, z)
        parts = cut(inverse)
        pull = jnp.broadcast_to(pulls[b], (8, full))
        half = dot3(cut(pull), parts)
        shift_row = dot3(cut(half), parts)[:1] / norms[b]
        spread = math.sqrt(ensemble - 1) * lax.rsqrt(norms[b])
        transposed = spread * inverse + jnp.where(live_line, shift_row, 0.0)
        t_out[b] = transposed.astype(BF16).reshape(ranks, PAD, full)

    t_copies = []
    for j, peer in enumerate(peers):
        copy = remote(
            t_out.at[:, peer], t_in.at[rank], t_send.at[j], t_recv.at[j], (me, peer)
        )
        t_copies.append(copy)
        copy.start()
    t_in[rank] = t_out[:, rank]

    arrive(state_copies[1:])
    start(state_passed)
    arrive(t_copies + state_copies[:1] + state_passed)

    piece_row = lax.broadcasted_iota(jnp.int32, (PAD, full), 0)
    for s in range(LIVE_MAX):
        weights = t_in[s % ranks, s // ranks]
        weights = jnp.where(piece_row == members, jnp.ones_like(weights), weights)
        keep = 1.0 - jnp.sum(weights.astype(F32), axis=1, keepdims=True)
        blended = dot(weights, states[s].reshape(full, width))
        mean = blended[members : members + 1, :] / ensemble
        value = (blended + keep * mean)[:members]
        is_live = new_start + s < new_end
        out_ref[s] = jnp.where(is_live, value, 0.0).astype(BF16)
    for s in range(LIVE_MAX, capacity):
        out_ref[s] = jnp.zeros((members, width), BF16)

    for k, offset in enumerate(OFFSETS):
        target = me + offset

        @pl.when((target >= 0) & (target < devices))
        def _(copy=halo_copies[k]):
            copy.wait_send()

    for side, offset in ((0, -1), (1, 1)):
        target = me + offset

        @pl.when((target >= 0) & (target < devices))
        def _(copy=mig_copies[side]):
            copy.wait_send()

    gathers = own_copies + own_passed + far_copies + far_passed + state_copies + state_passed
    for copy in gathers + t_copies:
        copy.wait_send()


def shards(devices, ranks, background, obs_ens, innovation, precision, loc_weight, old_split,
           new_split, obs_count, halo_tiles, region_list):
    capacity, members, width = background.shape
    obs_slots = obs_ens.shape[2]
    full = PAD * ranks
    halo_count = HPEER * HCAP
    per_rank = -(-LIVE_MAX // ranks)
    smem = pl.BlockSpec(memory_space=pltpu.SMEM)
    vmem = pl.BlockSpec(memory_space=pltpu.VMEM)
    count = len(OFFSETS)
    dma = pltpu.SemaphoreType.DMA
    return pl.pallas_call(
        functools.partial(kernel, devices, ranks),
        out_shape=jax.ShapeDtypeStruct((capacity, members, width), BF16),
        in_specs=[smem] * 6 + [vmem] * 4,
        out_specs=vmem,
        scratch_shapes=[
            pltpu.VMEM((LIVE_MAX, PAD, obs_slots), BF16),
            pltpu.VMEM((capacity, members, width), BF16),
            pltpu.VMEM((LIVE_MAX + halo_count, ranks, PAD, obs_slots), BF16),
            pltpu.VMEM((count, HCAP, PAD, obs_slots), BF16),
            pltpu.VMEM((count, HCAP, PAD, obs_slots), BF16),
            pltpu.VMEM((2, MOVE, members, width), BF16),
            pltpu.VMEM((2, MOVE, members, width), BF16),
            pltpu.VMEM((LIVE_MAX, ranks, PAD, width), BF16),
            pltpu.VMEM((per_rank, full, full), F32),
            pltpu.VMEM((per_rank, full, full), F32),
            pltpu.VMEM((per_rank, full, full), F32),
            pltpu.VMEM((per_rank, ranks, PAD, full), BF16),
            pltpu.VMEM((ranks, per_rank, PAD, full), BF16),
            dma((count,)),
            dma((count,)),
            dma((2,)),
            dma((2,)),
            dma((ranks - 1,)),
            dma((ranks - 1,)),
            dma((ranks - 1,)),
            dma((ranks - 1,)),
            dma((ranks - 1,)),
            dma((ranks - 1,)),
            dma((ranks - 1,)),
            dma((ranks - 1,)),
        ],
        compiler_params=pltpu.CompilerParams(collective_id=0, has_side_effects=True),
        cost_estimate=pl.CostEstimate(flops=10**8, bytes_accessed=10**7, transcendentals=0),
    )(old_split, new_split, obs_count, halo_tiles, region_list.T, loc_weight.T,
      jnp.swapaxes(background, 0, 1), jnp.swapaxes(obs_ens, 0, 1), innovation, precision)


def solution(mesh):
    in_specs = (
        P("tile", "mem", None),
        P("tile", "mem", None),
        P("tile", None),
        P("tile", None),
        P("tile", None),
        P(),
        P(),
        P("tile"),
        P(),
        P("tile", None),
    )
    out_specs = P("tile", "mem", None)
    body = functools.partial(shards, mesh.shape["tile"], mesh.shape["mem"])
    return jax.shard_map(body, mesh=mesh, in_specs=in_specs, out_specs=out_specs, check_vma=False)
```

```python
import functools
import math

import jax
import jax.numpy as jnp
from jax import lax
from jax.experimental import pallas as pl
from jax.experimental.pallas import tpu as pltpu
from jax.sharding import PartitionSpec as P

TILE_MEAN = 8
MOVE = 2
REACH = 3
HPEER = 3
HCAP = 4
NS_ITERS = 6
LIVE_MIN = TILE_MEAN - MOVE
LIVE_MAX = TILE_MEAN + MOVE
INFLATION = 1.1
PAD = 24
MESH = pl.DeviceIdType.MESH
F32 = jnp.float32
BF16 = jnp.bfloat16
OFFSETS = tuple(range(-REACH, 0)) + tuple(range(1, REACH + 1))


def dot(a, b):
    return jnp.dot(a, b, preferred_element_type=F32)


def cut(a):
    high = a.astype(BF16)
    return high, (a - high.astype(F32)).astype(BF16)


def dot3(a, b):
    ah, al = a
    bh, bl = b
    rows = ah.shape[0]
    both = dot(jnp.concatenate([ah, al], axis=0), bh)
    return both[:rows] + (dot(ah, bl) + both[rows:])


def kernel(
    devices,
    ranks,
    old_ref,
    new_ref,
    count_ref,
    halo_ref,
    region_ref,
    weight_ref,
    back_ref,
    obs_ref,
    innov_ref,
    prec_ref,
    out_ref,
    mine,
    out_t,
    back_t,
    table,
    stage,
    arrived,
    mig_out,
    mig_in,
    states,
    gram_s,
    y_s,
    z_s,
    t_out,
    t_in,
    halo_send,
    halo_recv,
    mig_send,
    mig_recv,
    own_send,
    own_recv,
    far_send,
    far_recv,
    state_send,
    state_recv,
    t_send,
    t_recv,
):
    members, capacity, width = back_ref.shape
    obs_slots = obs_ref.shape[2]
    ensemble = members * ranks
    full = PAD * ranks
    halo_count = HPEER * HCAP
    per_rank = -(-LIVE_MAX // ranks)
    me = lax.axis_index("tile")
    rank = lax.axis_index("mem")
    peers = [lax.rem(rank + j, ranks) for j in range(1, ranks)]

    barrier = pltpu.get_barrier_semaphore()
    for offset in OFFSETS:
        target = me + offset

        @pl.when((target >= 0) & (target < devices))
        def _():
            pl.semaphore_signal(barrier, inc=1, device_id=(target, rank), device_id_type=MESH)

    for peer in peers:
        pl.semaphore_signal(barrier, inc=1, device_id=(me, peer), device_id_type=MESH)

    old_start, old_end = old_ref[me], old_ref[me + 1]
    new_start, new_end = new_ref[me], new_ref[me + 1]
    row_id = lax.broadcasted_iota(jnp.int32, (PAD, obs_slots), 0)
    lane_id = lax.broadcasted_iota(jnp.int32, (1, obs_slots), 1)

    obs_all = obs_ref[...].astype(F32)
    for s in range(LIVE_MAX):
        live = (lane_id < count_ref[s]).astype(F32)
        root = jnp.sqrt(prec_ref[s : s + 1, :] * live)
        pulled = root * innov_ref[s : s + 1, :]
        rows = obs_all[:, s, :] * root
        fill = jnp.zeros((PAD - members, obs_slots), F32)
        block = jnp.concatenate([rows, fill], axis=0)
        block = jnp.where(row_id == members, pulled, block).astype(BF16)
        mine[s] = block
        table[s, rank] = block

    for k, offset in enumerate(OFFSETS):
        reader = jnp.clip(me + offset, 0, devices - 1)
        for c in range(HCAP):
            index = jnp.int32(0)
            for g in range(HPEER):
                first = halo_ref[reader, g * HCAP]
                here = (first >= new_start) & (first < new_end)
                index += jnp.where(here, halo_ref[reader, g * HCAP + c] - new_start, 0)
            index = jnp.clip(index, 0, LIVE_MAX - 1)
            stage[k, c] = mine[index]

    for s in range(LIVE_MAX):
        states[s, rank, members:] = jnp.zeros((PAD - members, width), BF16)

    signals = ranks - 1
    for offset in OFFSETS:
        inside = (me + offset >= 0) & (me + offset < devices)
        signals += jnp.where(inside, 1, 0)
    pl.semaphore_wait(barrier, signals)

    def remote(src, dst, send, recv, target):
        return pltpu.make_async_remote_copy(
            src_ref=src,
            dst_ref=dst,
            send_sem=send,
            recv_sem=recv,
            device_id=target,
            device_id_type=MESH,
        )

    halo_copies = []
    for k, offset in enumerate(OFFSETS):
        target = me + offset
        back_slot = len(OFFSETS) - 1 - k
        copy = remote(
            stage.at[k], arrived.at[back_slot], halo_send.at[k], halo_recv.at[back_slot],
            (target, rank),
        )
        source = me + OFFSETS[back_slot]
        halo_copies.append(copy)

        @pl.when((target >= 0) & (target < devices))
        def _(copy=copy):
            copy.start()

    own_rows = pl.ds(0, LIVE_MAX)
    far_rows = pl.ds(LIVE_MAX, halo_count)
    pair = rank + 1 - 2 * lax.rem(rank, 2)
    half_ranks = ranks // 2

    def gather(piece, send, recv):
        here = piece(rank)
        direct = [remote(here, here, send.at[0], recv.at[0], (me, pair))]
        passed = []
        for j in range(1, half_ranks):
            ahead = lax.rem(rank + 2 * j, ranks)
            behind = piece(lax.rem(rank + ranks - 2 * j, ranks))
            direct.append(remote(here, here, send.at[j], recv.at[j], (me, ahead)))
            k = half_ranks + j - 1
            passed.append(remote(behind, behind, send.at[k], recv.at[k], (me, pair)))
        return direct, passed

    def start(copies):
        for copy in copies:
            copy.start()

    def arrive(copies):
        for copy in copies:
            copy.wait_recv()

    own_copies, own_passed = gather(lambda r: table.at[own_rows, r], own_send, own_recv)
    far_copies, far_passed = gather(lambda r: table.at[far_rows, r], far_send, far_recv)
    sure = LIVE_MIN - 2 * MOVE
    chunks = ((MOVE, sure), (0, MOVE), (MOVE + sure, LIVE_MAX - MOVE - sure))
    pieces = [
        gather(
            lambda r, a=a, c=c: states.at[pl.ds(a, c), r],
            state_send.at[i],
            state_recv.at[i],
        )
        for i, (a, c) in enumerate(chunks)
    ]
    state_copies, state_passed = pieces[1][0] + pieces[2][0], pieces[1][1] + pieces[2][1]
    start(own_copies[::-1])

    back_all = back_ref[...].astype(F32)
    for s in range(capacity):
        back_t[s] = back_all[:, s, :].astype(BF16)
    for s in range(MOVE, MOVE + sure):
        own = back_t[jnp.clip(new_start + s - old_start, 0, capacity - 1)]
        states[s, rank, :members] = own
    old_count = old_end - old_start
    for c in range(MOVE):
        mig_out[0, c] = back_t[jnp.clip(c, 0, capacity - 1)]
        mig_out[1, c] = back_t[jnp.clip(old_count - MOVE + c, 0, capacity - 1)]
    mig_copies = []
    for side, offset in ((0, -1), (1, 1)):
        target = me + offset
        copy = remote(
            mig_out.at[side], mig_in.at[1 - side], mig_send.at[side], mig_recv.at[1 - side],
            (target, rank),
        )
        mig_copies.append(copy)

        @pl.when((target >= 0) & (target < devices))
        def _(copy=copy):
            copy.start()

    start(pieces[0][0][::-1])

    for k, offset in enumerate(OFFSETS):
        back_slot = len(OFFSETS) - 1 - k
        source = me + OFFSETS[back_slot]

        @pl.when((source >= 0) & (source < devices))
        def _(copy=halo_copies[k]):
            copy.wait_recv()

    for g in range(HPEER):
        first = halo_ref[me, g * HCAP]
        owner = jnp.int32(0)
        for k, offset in enumerate(OFFSETS):
            source = jnp.clip(me + offset, 0, devices - 1)
            held = (first >= new_ref[source]) & (first < new_ref[source + 1])
            inside = (me + offset >= 0) & (me + offset < devices)
            owner = jnp.where(held & inside, k, owner)
        for c in range(HCAP):
            table[LIVE_MAX + g * HCAP + c, rank] = arrived[owner, c]
    start(far_copies[::-1])

    for side, offset in ((0, -1), (1, 1)):
        source = me - offset

        @pl.when((source >= 0) & (source < devices))
        def _(copy=mig_copies[side]):
            copy.wait_recv()

    for s in list(range(MOVE)) + list(range(MOVE + sure, LIVE_MAX)):
        position = new_start + s
        left = mig_in[0, jnp.clip(position - old_start + MOVE, 0, MOVE - 1)]
        own = back_t[jnp.clip(position - old_start, 0, capacity - 1)]
        right = mig_in[1, jnp.clip(position - old_end, 0, MOVE - 1)]
        row = jnp.where(position < old_start, left, jnp.where(position < old_end, own, right))
        states[s, rank, :members] = row
    start(state_copies[::-1])

    arrive(own_copies[1:])
    start(own_passed)
    arrive(far_copies[1:])
    start(far_passed)
    arrive(pieces[0][0][1:])
    start(pieces[0][1])
    arrive(own_copies[:1] + own_passed + far_copies[:1] + far_passed)

    grid_row = lax.broadcasted_iota(jnp.int32, (full, full), 0)
    grid_col = lax.broadcasted_iota(jnp.int32, (full, full), 1)
    live_row = lax.rem(grid_row, PAD) < members
    live_col = lax.rem(grid_col, PAD) < members
    unit = (grid_row == grid_col).astype(F32)
    live_unit = jnp.where(live_row, unit, 0.0)
    line = lax.broadcasted_iota(jnp.int32, (1, full), 1)
    live_line = lax.rem(line, PAD) < members
    shift = (ensemble - 1) / INFLATION
    entries = region_ref.shape[0] + 1

    norms, pulls = [], []
    for b in range(per_rank):
        slot = jnp.minimum(rank + b * ranks, LIVE_MAX - 1)
        gram = jnp.zeros((full, full), F32)
        for e in range(entries):
            if e == 0:
                index = slot
            else:
                named = region_ref[e - 1, slot]
                index = jnp.where(named < capacity, named, named - capacity + LIVE_MAX)
            index = jnp.clip(index, 0, LIVE_MAX + halo_count - 1)
            block = table[index].reshape(full, obs_slots)
            product = lax.dot_general(
                block, block, (((1,), (1,)), ((), ())), preferred_element_type=F32
            )
            gram += product if e == 0 else weight_ref[e - 1, slot] * product
        pulls.append(jnp.where(live_line, gram[members : members + 1, :], 0.0))
        system = jnp.where(live_row & live_col, gram, 0.0) + shift * live_unit
        total = jnp.sum(jnp.sum(system * system, axis=1, keepdims=True), axis=0, keepdims=True)
        norm = jnp.sqrt(total)
        norms.append(norm)
        y = system / norm
        middle = 1.5 * unit - 0.5 * y
        y_s[b] = dot3(cut(y), cut(middle))
        z_s[b] = middle

    def step(_, carry):
        middles = []
        for b in range(per_rank):
            middles.append(cut(1.5 * unit - 0.5 * dot3(cut(z_s[b]), cut(y_s[b]))))
        for b in range(per_rank):
            y_s[b] = dot3(cut(y_s[b]), middles[b])
            z_s[b] = dot3(middles[b], cut(z_s[b]))
        return carry

    lax.fori_loop(0, NS_ITERS - 2, step, 0)
    for b in range(per_rank):
        z = cut(z_s[b])
        middle = cut(1.5 * unit - 0.5 * dot3(z, cut(y_s[b])))
        inverse = dot3(middle, z)
        parts = cut(inverse)
        pull = jnp.broadcast_to(pulls[b], (16, full))
        half = dot3(cut(pull), parts)
        shift_row = dot3(cut(half), parts)[:1] / norms[b]
        spread = math.sqrt(ensemble - 1) * lax.rsqrt(norms[b])
        transposed = spread * inverse + jnp.where(live_line, shift_row, 0.0)
        t_out[b] = transposed.astype(BF16).reshape(ranks, PAD, full)

    t_copies = []
    for j, peer in enumerate(peers):
        copy = remote(
            t_out.at[:, peer], t_in.at[rank], t_send.at[j], t_recv.at[j], (me, peer)
        )
        t_copies.append(copy)
        copy.start()
    t_in[rank] = t_out[:, rank]

    for direct, passed in pieces[1:]:
        arrive(direct[1:])
        start(passed)
    arrive(t_copies + pieces[0][0][:1] + pieces[0][1])
    for direct, passed in pieces[1:]:
        arrive(direct[:1] + passed)

    values = []
    piece_row = lax.broadcasted_iota(jnp.int32, (PAD, full), 0)
    for s in range(LIVE_MAX):
        weights = t_in[s % ranks, s // ranks]
        weights = jnp.where(piece_row == members, jnp.ones_like(weights), weights)
        keep = 1.0 - jnp.sum(weights.astype(F32), axis=1, keepdims=True)
        blended = dot(weights, states[s].reshape(full, width))
        mean = blended[members : members + 1, :] / ensemble
        value = (blended + keep * mean)[:members]
        is_live = new_start + s < new_end
        values.append(jnp.where(is_live, value, 0.0))
    values += [jnp.zeros((members, width), F32)] * (capacity - LIVE_MAX)
    for s, value in enumerate(values):
        out_t[:, s, :] = value
    out_ref[...] = out_t[...].astype(BF16)

    for k, offset in enumerate(OFFSETS):
        target = me + offset

        @pl.when((target >= 0) & (target < devices))
        def _(copy=halo_copies[k]):
            copy.wait_send()

    for side, offset in ((0, -1), (1, 1)):
        target = me + offset

        @pl.when((target >= 0) & (target < devices))
        def _(copy=mig_copies[side]):
            copy.wait_send()

    gathers = own_copies + own_passed + far_copies + far_passed + pieces[0][0] + pieces[0][1]
    gathers += state_copies + state_passed
    for copy in gathers + t_copies:
        copy.wait_send()


def shards(devices, ranks, background, obs_ens, innovation, precision, loc_weight, old_split,
           new_split, obs_count, halo_tiles, region_list):
    capacity, members, width = background.shape
    obs_slots = obs_ens.shape[2]
    full = PAD * ranks
    halo_count = HPEER * HCAP
    per_rank = -(-LIVE_MAX // ranks)
    smem = pl.BlockSpec(memory_space=pltpu.SMEM)
    vmem = pl.BlockSpec(memory_space=pltpu.VMEM)
    count = len(OFFSETS)
    dma = pltpu.SemaphoreType.DMA
    result = pl.pallas_call(
        functools.partial(kernel, devices, ranks),
        out_shape=jax.ShapeDtypeStruct((members, capacity, width), BF16),
        in_specs=[smem] * 6 + [vmem] * 4,
        out_specs=vmem,
        scratch_shapes=[
            pltpu.VMEM((LIVE_MAX, PAD, obs_slots), BF16),
            pltpu.VMEM((members, capacity, width), F32),
            pltpu.VMEM((capacity, members, width), BF16),
            pltpu.VMEM((LIVE_MAX + halo_count, ranks, PAD, obs_slots), BF16),
            pltpu.VMEM((count, HCAP, PAD, obs_slots), BF16),
            pltpu.VMEM((count, HCAP, PAD, obs_slots), BF16),
            pltpu.VMEM((2, MOVE, members, width), BF16),
            pltpu.VMEM((2, MOVE, members, width), BF16),
            pltpu.VMEM((LIVE_MAX, ranks, PAD, width), BF16),
            pltpu.VMEM((per_rank, full, full), F32),
            pltpu.VMEM((per_rank, full, full), F32),
            pltpu.VMEM((per_rank, full, full), F32),
            pltpu.VMEM((per_rank, ranks, PAD, full), BF16),
            pltpu.VMEM((ranks, per_rank, PAD, full), BF16),
            dma((count,)),
            dma((count,)),
            dma((2,)),
            dma((2,)),
            dma((ranks - 1,)),
            dma((ranks - 1,)),
            dma((ranks - 1,)),
            dma((ranks - 1,)),
            dma((3, ranks - 1)),
            dma((3, ranks - 1)),
            dma((ranks - 1,)),
            dma((ranks - 1,)),
        ],
        compiler_params=pltpu.CompilerParams(collective_id=0, has_side_effects=True),
        cost_estimate=pl.CostEstimate(flops=10**8, bytes_accessed=10**7, transcendentals=0),
    )(old_split, new_split, obs_count, halo_tiles, region_list.T, loc_weight.T,
      jnp.swapaxes(background, 0, 1), jnp.swapaxes(obs_ens, 0, 1), innovation, precision)
    return jnp.swapaxes(result, 0, 1)


def solution(mesh):
    in_specs = (
        P("tile", "mem", None),
        P("tile", "mem", None),
        P("tile", None),
        P("tile", None),
        P("tile", None),
        P(),
        P(),
        P("tile"),
        P(),
        P("tile", None),
    )
    out_specs = P("tile", "mem", None)
    body = functools.partial(shards, mesh.shape["tile"], mesh.shape["mem"])
    return jax.shard_map(body, mesh=mesh, in_specs=in_specs, out_specs=out_specs, check_vma=False)
```

```python
import functools
import math

import jax
import jax.numpy as jnp
from jax import lax
from jax.experimental import pallas as pl
from jax.experimental.pallas import tpu as pltpu
from jax.sharding import PartitionSpec as P

TILE_MEAN = 8
MOVE = 2
REACH = 3
HPEER = 3
HCAP = 4
NS_ITERS = 6
LIVE_MIN = TILE_MEAN - MOVE
LIVE_MAX = TILE_MEAN + MOVE
INFLATION = 1.1
PAD = 24
MESH = pl.DeviceIdType.MESH
F32 = jnp.float32
BF16 = jnp.bfloat16
OFFSETS = tuple(range(-REACH, 0)) + tuple(range(1, REACH + 1))


def dot(a, b):
    return jnp.dot(a, b, preferred_element_type=F32)


def cut(a):
    high = a.astype(BF16)
    return high, (a - high.astype(F32)).astype(BF16)


def dot3(a, b):
    ah, al = a
    bh, bl = b
    rows = ah.shape[0]
    both = dot(jnp.concatenate([ah, al], axis=0), bh)
    return both[:rows] + (dot(ah, bl) + both[rows:])


def kernel(
    devices,
    ranks,
    old_ref,
    new_ref,
    count_ref,
    halo_ref,
    region_ref,
    weight_ref,
    back_ref,
    obs_ref,
    innov_ref,
    prec_ref,
    out_ref,
    mine,
    back_t,
    table,
    stage,
    arrived,
    mig_out,
    mig_in,
    states,
    gram_s,
    y_s,
    z_s,
    t_out,
    t_in,
    halo_send,
    halo_recv,
    mig_send,
    mig_recv,
    own_send,
    own_recv,
    far_send,
    far_recv,
    state_send,
    state_recv,
    t_send,
    t_recv,
):
    members, capacity, width = back_ref.shape
    obs_slots = obs_ref.shape[2]
    ensemble = members * ranks
    full = PAD * ranks
    halo_count = HPEER * HCAP
    per_rank = -(-LIVE_MAX // ranks)
    me = lax.axis_index("tile")
    rank = lax.axis_index("mem")
    peers = [lax.rem(rank + j, ranks) for j in range(1, ranks)]

    barrier = pltpu.get_barrier_semaphore()
    for offset in OFFSETS:
        target = me + offset

        @pl.when((target >= 0) & (target < devices))
        def _():
            pl.semaphore_signal(barrier, inc=1, device_id=(target, rank), device_id_type=MESH)

    for peer in peers:
        pl.semaphore_signal(barrier, inc=1, device_id=(me, peer), device_id_type=MESH)

    old_start, old_end = old_ref[me], old_ref[me + 1]
    new_start, new_end = new_ref[me], new_ref[me + 1]
    row_id = lax.broadcasted_iota(jnp.int32, (PAD, obs_slots), 0)
    lane_id = lax.broadcasted_iota(jnp.int32, (1, obs_slots), 1)

    obs_all = obs_ref[...].astype(F32)
    for s in range(LIVE_MAX):
        live = (lane_id < count_ref[s]).astype(F32)
        root = jnp.sqrt(prec_ref[s : s + 1, :] * live)
        pulled = root * innov_ref[s : s + 1, :]
        rows = obs_all[:, s, :] * root
        fill = jnp.zeros((PAD - members, obs_slots), F32)
        block = jnp.concatenate([rows, fill], axis=0)
        block = jnp.where(row_id == members, pulled, block).astype(BF16)
        mine[s] = block
        table[s, rank] = block

    for k, offset in enumerate(OFFSETS):
        reader = jnp.clip(me + offset, 0, devices - 1)
        for c in range(HCAP):
            index = jnp.int32(0)
            for g in range(HPEER):
                first = halo_ref[reader, g * HCAP]
                here = (first >= new_start) & (first < new_end)
                index += jnp.where(here, halo_ref[reader, g * HCAP + c] - new_start, 0)
            index = jnp.clip(index, 0, LIVE_MAX - 1)
            stage[k, c] = mine[index]

    for s in range(LIVE_MAX):
        states[s, rank, members:] = jnp.zeros((PAD - members, width), BF16)

    signals = ranks - 1
    for offset in OFFSETS:
        inside = (me + offset >= 0) & (me + offset < devices)
        signals += jnp.where(inside, 1, 0)
    pl.semaphore_wait(barrier, signals)

    def remote(src, dst, send, recv, target):
        return pltpu.make_async_remote_copy(
            src_ref=src,
            dst_ref=dst,
            send_sem=send,
            recv_sem=recv,
            device_id=target,
            device_id_type=MESH,
        )

    halo_copies = []
    for k, offset in enumerate(OFFSETS):
        target = me + offset
        back_slot = len(OFFSETS) - 1 - k
        copy = remote(
            stage.at[k], arrived.at[back_slot], halo_send.at[k], halo_recv.at[back_slot],
            (target, rank),
        )
        source = me + OFFSETS[back_slot]
        halo_copies.append(copy)

        @pl.when((target >= 0) & (target < devices))
        def _(copy=copy):
            copy.start()

    own_rows = pl.ds(0, LIVE_MAX)
    far_rows = pl.ds(LIVE_MAX, halo_count)
    pair = rank + 1 - 2 * lax.rem(rank, 2)
    half_ranks = ranks // 2

    def gather(piece, send, recv):
        here = piece(rank)
        direct = [remote(here, here, send.at[0], recv.at[0], (me, pair))]
        passed = []
        for j in range(1, half_ranks):
            ahead = lax.rem(rank + 2 * j, ranks)
            behind = piece(lax.rem(rank + ranks - 2 * j, ranks))
            direct.append(remote(here, here, send.at[j], recv.at[j], (me, ahead)))
            k = half_ranks + j - 1
            passed.append(remote(behind, behind, send.at[k], recv.at[k], (me, pair)))
        return direct, passed

    def start(copies):
        for copy in copies:
            copy.start()

    def arrive(copies):
        for copy in copies:
            copy.wait_recv()

    own_copies, own_passed = gather(lambda r: table.at[own_rows, r], own_send, own_recv)
    far_copies, far_passed = gather(lambda r: table.at[far_rows, r], far_send, far_recv)
    sure = LIVE_MIN - 2 * MOVE
    chunks = ((MOVE, sure), (0, MOVE), (MOVE + sure, LIVE_MAX - MOVE - sure))
    pieces = [
        gather(
            lambda r, a=a, c=c: states.at[pl.ds(a, c), r],
            state_send.at[i],
            state_recv.at[i],
        )
        for i, (a, c) in enumerate(chunks)
    ]
    state_copies, state_passed = pieces[1][0] + pieces[2][0], pieces[1][1] + pieces[2][1]
    start(own_copies[::-1])

    back_all = back_ref[...].astype(F32)
    for s in range(capacity):
        back_t[s] = back_all[:, s, :].astype(BF16)
    for s in range(MOVE, MOVE + sure):
        own = back_t[jnp.clip(new_start + s - old_start, 0, capacity - 1)]
        states[s, rank, :members] = own
    old_count = old_end - old_start
    for c in range(MOVE):
        mig_out[0, c] = back_t[jnp.clip(c, 0, capacity - 1)]
        mig_out[1, c] = back_t[jnp.clip(old_count - MOVE + c, 0, capacity - 1)]
    mig_copies = []
    for side, offset in ((0, -1), (1, 1)):
        target = me + offset
        copy = remote(
            mig_out.at[side], mig_in.at[1 - side], mig_send.at[side], mig_recv.at[1 - side],
            (target, rank),
        )
        mig_copies.append(copy)

        @pl.when((target >= 0) & (target < devices))
        def _(copy=copy):
            copy.start()

    start(pieces[0][0][::-1])

    for k, offset in enumerate(OFFSETS):
        back_slot = len(OFFSETS) - 1 - k
        source = me + OFFSETS[back_slot]

        @pl.when((source >= 0) & (source < devices))
        def _(copy=halo_copies[k]):
            copy.wait_recv()

    for g in range(HPEER):
        first = halo_ref[me, g * HCAP]
        owner = jnp.int32(0)
        for k, offset in enumerate(OFFSETS):
            source = jnp.clip(me + offset, 0, devices - 1)
            held = (first >= new_ref[source]) & (first < new_ref[source + 1])
            inside = (me + offset >= 0) & (me + offset < devices)
            owner = jnp.where(held & inside, k, owner)
        for c in range(HCAP):
            table[LIVE_MAX + g * HCAP + c, rank] = arrived[owner, c]
    start(far_copies[::-1])

    for side, offset in ((0, -1), (1, 1)):
        source = me - offset

        @pl.when((source >= 0) & (source < devices))
        def _(copy=mig_copies[side]):
            copy.wait_recv()

    for s in list(range(MOVE)) + list(range(MOVE + sure, LIVE_MAX)):
        position = new_start + s
        left = mig_in[0, jnp.clip(position - old_start + MOVE, 0, MOVE - 1)]
        own = back_t[jnp.clip(position - old_start, 0, capacity - 1)]
        right = mig_in[1, jnp.clip(position - old_end, 0, MOVE - 1)]
        row = jnp.where(position < old_start, left, jnp.where(position < old_end, own, right))
        states[s, rank, :members] = row
    start(state_copies[::-1])

    arrive(own_copies[1:])
    start(own_passed)
    arrive(far_copies[1:])
    start(far_passed)
    arrive(pieces[0][0][1:])
    start(pieces[0][1])
    arrive(own_copies[:1] + own_passed + far_copies[:1] + far_passed)

    grid_row = lax.broadcasted_iota(jnp.int32, (full, full), 0)
    grid_col = lax.broadcasted_iota(jnp.int32, (full, full), 1)
    live_row = lax.rem(grid_row, PAD) < members
    live_col = lax.rem(grid_col, PAD) < members
    unit = (grid_row == grid_col).astype(F32)
    live_unit = jnp.where(live_row, unit, 0.0)
    line = lax.broadcasted_iota(jnp.int32, (1, full), 1)
    live_line = lax.rem(line, PAD) < members
    shift = (ensemble - 1) / INFLATION
    entries = region_ref.shape[0] + 1

    norms, pulls = [], []
    for b in range(per_rank):
        slot = jnp.minimum(rank + b * ranks, LIVE_MAX - 1)
        gram = jnp.zeros((full, full), F32)
        for e in range(entries):
            if e == 0:
                index = slot
            else:
                named = region_ref[e - 1, slot]
                index = jnp.where(named < capacity, named, named - capacity + LIVE_MAX)
            index = jnp.clip(index, 0, LIVE_MAX + halo_count - 1)
            block = table[index].reshape(full, obs_slots)
            product = lax.dot_general(
                block, block, (((1,), (1,)), ((), ())), preferred_element_type=F32
            )
            gram += product if e == 0 else weight_ref[e - 1, slot] * product
        pulls.append(jnp.where(live_line, gram[members : members + 1, :], 0.0))
        system = jnp.where(live_row & live_col, gram, 0.0) + shift * live_unit
        total = jnp.sum(jnp.sum(system * system, axis=1, keepdims=True), axis=0, keepdims=True)
        norm = jnp.sqrt(total)
        norms.append(norm)
        y = system / norm
        middle = 1.5 * unit - 0.5 * y
        y_s[b] = dot3(cut(y), cut(middle))
        z_s[b] = middle

    def step(_, carry):
        middles = []
        for b in range(per_rank):
            middles.append(cut(1.5 * unit - 0.5 * dot3(cut(z_s[b]), cut(y_s[b]))))
        for b in range(per_rank):
            y_s[b] = dot3(cut(y_s[b]), middles[b])
            z_s[b] = dot3(middles[b], cut(z_s[b]))
        return carry

    lax.fori_loop(0, NS_ITERS - 2, step, 0)
    for b in range(per_rank):
        z = cut(z_s[b])
        middle = cut(1.5 * unit - 0.5 * dot3(z, cut(y_s[b])))
        inverse = dot3(middle, z)
        parts = cut(inverse)
        pull = jnp.broadcast_to(pulls[b], (16, full))
        half = dot3(cut(pull), parts)
        shift_row = dot3(cut(half), parts)[:1] / norms[b]
        spread = math.sqrt(ensemble - 1) * lax.rsqrt(norms[b])
        transposed = spread * inverse + jnp.where(live_line, shift_row, 0.0)
        t_out[b] = transposed.astype(BF16).reshape(ranks, PAD, full)

    t_copies = []
    for j, peer in enumerate(peers):
        copy = remote(
            t_out.at[:, peer], t_in.at[rank], t_send.at[j], t_recv.at[j], (me, peer)
        )
        t_copies.append(copy)
        copy.start()
    t_in[rank] = t_out[:, rank]

    for direct, passed in pieces[1:]:
        arrive(direct[1:])
        start(passed)
    arrive(t_copies + pieces[0][0][:1] + pieces[0][1])
    for direct, passed in pieces[1:]:
        arrive(direct[:1] + passed)

    piece_row = lax.broadcasted_iota(jnp.int32, (PAD, full), 0)
    for s in range(LIVE_MAX):
        weights = t_in[s % ranks, s // ranks]
        weights = jnp.where(piece_row == members, jnp.ones_like(weights), weights)
        keep = 1.0 - jnp.sum(weights.astype(F32), axis=1, keepdims=True)
        blended = dot(weights, states[s].reshape(full, width))
        mean = blended[members : members + 1, :] / ensemble
        value = (blended + keep * mean)[:members]
        is_live = new_start + s < new_end
        out_ref[s] = jnp.where(is_live, value, 0.0).astype(BF16)
    for s in range(LIVE_MAX, capacity):
        out_ref[s] = jnp.zeros((members, width), BF16)

    for k, offset in enumerate(OFFSETS):
        target = me + offset

        @pl.when((target >= 0) & (target < devices))
        def _(copy=halo_copies[k]):
            copy.wait_send()

    for side, offset in ((0, -1), (1, 1)):
        target = me + offset

        @pl.when((target >= 0) & (target < devices))
        def _(copy=mig_copies[side]):
            copy.wait_send()

    gathers = own_copies + own_passed + far_copies + far_passed + pieces[0][0] + pieces[0][1]
    gathers += state_copies + state_passed
    for copy in gathers + t_copies:
        copy.wait_send()


def shards(devices, ranks, background, obs_ens, innovation, precision, loc_weight, old_split,
           new_split, obs_count, halo_tiles, region_list):
    capacity, members, width = background.shape
    obs_slots = obs_ens.shape[2]
    full = PAD * ranks
    halo_count = HPEER * HCAP
    per_rank = -(-LIVE_MAX // ranks)
    smem = pl.BlockSpec(memory_space=pltpu.SMEM)
    vmem = pl.BlockSpec(memory_space=pltpu.VMEM)
    count = len(OFFSETS)
    dma = pltpu.SemaphoreType.DMA
    return pl.pallas_call(
        functools.partial(kernel, devices, ranks),
        out_shape=jax.ShapeDtypeStruct((capacity, members, width), BF16),
        in_specs=[smem] * 6 + [vmem] * 4,
        out_specs=vmem,
        scratch_shapes=[
            pltpu.VMEM((LIVE_MAX, PAD, obs_slots), BF16),
            pltpu.VMEM((capacity, members, width), BF16),
            pltpu.VMEM((LIVE_MAX + halo_count, ranks, PAD, obs_slots), BF16),
            pltpu.VMEM((count, HCAP, PAD, obs_slots), BF16),
            pltpu.VMEM((count, HCAP, PAD, obs_slots), BF16),
            pltpu.VMEM((2, MOVE, members, width), BF16),
            pltpu.VMEM((2, MOVE, members, width), BF16),
            pltpu.VMEM((LIVE_MAX, ranks, PAD, width), BF16),
            pltpu.VMEM((per_rank, full, full), F32),
            pltpu.VMEM((per_rank, full, full), F32),
            pltpu.VMEM((per_rank, full, full), F32),
            pltpu.VMEM((per_rank, ranks, PAD, full), BF16),
            pltpu.VMEM((ranks, per_rank, PAD, full), BF16),
            dma((count,)),
            dma((count,)),
            dma((2,)),
            dma((2,)),
            dma((ranks - 1,)),
            dma((ranks - 1,)),
            dma((ranks - 1,)),
            dma((ranks - 1,)),
            dma((3, ranks - 1)),
            dma((3, ranks - 1)),
            dma((ranks - 1,)),
            dma((ranks - 1,)),
        ],
        compiler_params=pltpu.CompilerParams(collective_id=0, has_side_effects=True),
        cost_estimate=pl.CostEstimate(flops=10**8, bytes_accessed=10**7, transcendentals=0),
    )(old_split, new_split, obs_count, halo_tiles, region_list.T, loc_weight.T,
      jnp.swapaxes(background, 0, 1), jnp.swapaxes(obs_ens, 0, 1), innovation, precision)


def solution(mesh):
    in_specs = (
        P("tile", "mem", None),
        P("tile", "mem", None),
        P("tile", None),
        P("tile", None),
        P("tile", None),
        P(),
        P(),
        P("tile"),
        P(),
        P("tile", None),
    )
    out_specs = P("tile", "mem", None)
    body = functools.partial(shards, mesh.shape["tile"], mesh.shape["mem"])
    return jax.shard_map(body, mesh=mesh, in_specs=in_specs, out_specs=out_specs, check_vma=False)
```
